32 devices in a mesh: gx: 8 (over z, x), gy: 4 (over y, core).
Axes of the slice: x: 2, y: 2, z: 4, core: 2. Of those that a mesh axis runs over, the one named last changes fastest.
Arguments:
- velocity: float32 [2, 1024, 1024], P(None, 'gy', 'gx'), may hold values from -3 to 3
- stress: float32 [3, 1024, 1024], P(None, 'gy', 'gx'), may hold values from -3 to 3
- ice_mass: float32 [1024, 1024], P('gy', 'gx'), may hold values from 0.5 to 4
- strength: float32 [1024, 1024], P('gy', 'gx'), may hold values from 0.2 to 2
- land_mask: int32 [1024, 1024], P('gy', 'gx'), may hold values from 0 to 1
- ocean_forcing: float32 [4, 1024, 1024], P(None, ('gy', 'gx')), may hold values from -3 to 3
Outputs:
- velocity_out: float32 [2, 1024, 1024], P(None, 'gy', 'gx')
- stress_out: float32 [3, 1024, 1024], P(None, 'gy', 'gx')
- residuals: float32 [4], replicated
- ocean_stress: float32 [2, 1024, 1024], P(None, ('gy', 'gx'))
The draws below stay inside these ranges and needn't reach their ends.
All inputs are finite; a program needn't handle non-finite values.
Results may differ from the reference program's by a relative error of at most 0.0001.
Values sent between devices are 32-bit elements; how exact they have to be, the bound alone decides.
A program may use at most 64 MiB of HBM per device.

```python
import math
import jax
import jax.numpy as jnp
from jax import lax

ITERS = 4
NX = 1024
NY = 1024


def draw_land_mask(key, part):
    lon_index = lax.broadcasted_iota(jnp.int32, (NY, NX), 1)
    lat_index = lax.broadcasted_iota(jnp.int32, (NY, NX), 0)
    threshold = 100 + 300 * lon_index // NX + 300 * lat_index // NY
    rolled = jax.random.randint(jax.random.fold_in(key, 17), (NY, NX), 0, 1000)
    return (rolled >= threshold).astype(jnp.int32)


def levels(stream_key, shape, pieces, low, largest):
    def one(axis_at, blocks):
        steps = jax.random.uniform(jax.random.fold_in(jax.random.fold_in(stream_key, 6), axis_at), (blocks,), jnp.float32, low / len(pieces), largest / len(pieces))
        return jnp.repeat(jnp.exp(steps), shape[axis_at] // blocks).reshape((-1,) + (1,) * (len(shape) - axis_at - 1))

    gain = one(*pieces[0])
    for cut in pieces[1:]:
        gain = gain * one(*cut)
    return gain


def normal_values(key, shape, deviation, bound, cuts=(), dtype=jnp.bfloat16):
    level = levels(key, shape, cuts, -0.22, 0.18) if cuts else 1.0
    values = jax.random.normal(key, shape, jnp.float32) * deviation * level
    return jnp.minimum(jnp.maximum(values, -bound), bound).astype(dtype)


def setup_inputs(seed: int = 0) -> dict:
    key_list = jax.random.split(jax.random.key(seed), 7)
    return {
        "velocity": normal_values(key_list[0], (2, NY, NX), 0.5, 3.0, ((1, 4), (2, 8)), jnp.float32),
        "stress": normal_values(key_list[1], (3, NY, NX), 0.5, 3.0, ((1, 4), (2, 8)), jnp.float32),
        "ice_mass": jnp.clip(jnp.exp(math.log(4.0) - 2.0794415 * jax.random.uniform(key_list[2], (NY, NX), jnp.float32) ** levels(key_list[2], (NY, NX), ((0, 4), (1, 8)), -0.2, 0.2)), 0.5, 4.0),
        "strength": jnp.clip(jnp.exp(math.log(2.0) - 2.3025851 * jax.random.uniform(key_list[3], (NY, NX), jnp.float32) ** levels(key_list[3], (NY, NX), ((0, 4), (1, 8)), -0.2, 0.2)), 0.2, 2.0),
        "land_mask": draw_land_mask(jax.random.fold_in(key_list[6], 71), 0),
        "ocean_forcing": normal_values(key_list[5], (4, NY, NX), 0.5, 3.0, ((1, 32),), jnp.float32),
    }


ALPHA = 4.0
BETA = 4.0
WATER_DRAG = 1.0
DELTA_FLOOR = 0.0025

def extend_field(field):
    wrapped = jnp.concatenate([field[..., -1:], field, field[..., :1]], axis=-1)
    padding = [(0, 0)] * (field.ndim - 2) + [(1, 1), (0, 0)]
    return jnp.pad(wrapped, padding)

def diff_east(padded):
    return 0.5 * (padded[..., 1:-1, 2:] - padded[..., 1:-1, :-2])

def diff_north(padded):
    return 0.5 * (padded[..., 2:, 1:-1] - padded[..., :-2, 1:-1])

def relax_stress(padded_vel, stress, strength, ice_frac):
    east_dx = diff_east(padded_vel[0])
    east_dy = diff_north(padded_vel[0])
    north_dx = diff_east(padded_vel[1])
    north_dy = diff_north(padded_vel[1])
    divergence = east_dx + north_dy
    tension = east_dx - north_dy
    shear_rate = east_dy + north_dx
    delta_rate = jnp.sqrt(divergence * divergence + 0.25 * (tension * tension + shear_rate * shear_rate) + DELTA_FLOOR)
    target = jnp.stack([strength * (divergence / delta_rate - 1.0), strength * tension / (4.0 * delta_rate), strength * shear_rate / (8.0 * delta_rate)])
    return (stress + (target - stress) / ALPHA) * ice_frac

def drag_coeff(vel, currents):
    east_gap = currents[0] - vel[0]
    north_gap = currents[1] - vel[1]
    return WATER_DRAG * jnp.sqrt(east_gap * east_gap + north_gap * north_gap + 0.01)

def relax_velocity(padded_stress, vel, vel_start, forcing, ice_mass, coriolis, ice_frac):
    normal_xx = 0.5 * (padded_stress[0] + padded_stress[1])
    normal_yy = 0.5 * (padded_stress[0] - padded_stress[1])
    shear_xy = padded_stress[2]
    force_east = diff_east(normal_xx) + diff_north(shear_xy)
    force_north = diff_east(shear_xy) + diff_north(normal_yy)
    drag_rate = drag_coeff(vel, forcing[2:4])
    denominator = BETA + 1.0 + drag_rate / ice_mass
    new_east = (BETA * vel[0] + vel_start[0] + (force_east + forcing[0] + drag_rate * forcing[2]) / ice_mass + coriolis * vel[1]) / denominator * ice_frac
    new_north = (BETA * vel[1] + vel_start[1] + (force_north + forcing[1] + drag_rate * forcing[3]) / ice_mass - coriolis * vel[0]) / denominator * ice_frac
    return jnp.stack([new_east, new_north])

def reference(velocity, stress, ice_mass, strength, land_mask, ocean_forcing):
    ice_frac = land_mask.astype(jnp.float32)
    lat_rows = jnp.arange(NY).astype(jnp.float32)
    coriolis = (0.3 + 1.2 * (lat_rows + 0.5) / NY)[:, None]
    vel = velocity
    history = []
    for subcycle in range(ITERS):
        stress = relax_stress(extend_field(vel), stress, strength, ice_frac)
        new_vel = relax_velocity(extend_field(stress), vel, velocity, ocean_forcing, ice_mass, coriolis, ice_frac)
        change = new_vel - vel
        history.append(jnp.sum(change * change))
        vel = new_vel
    drag_rate = drag_coeff(vel, ocean_forcing[2:4])
    ocean_stress = drag_rate * (vel - ocean_forcing[2:4]) * ice_frac
    return (vel, stress, jnp.stack(history), ocean_stress)
```

```python
import functools

import jax
import jax.numpy as jnp
from jax import lax
from jax.experimental import pallas as pl
from jax.experimental.pallas import tpu as pltpu
from jax.sharding import PartitionSpec as P

ITERS = 4
DELTA_FLOOR = 0.0025
PAD = 8
CH = 64
MESH = pl.DeviceIdType.MESH

WEST, EAST, SOUTH, NORTH, SW, SE, NW, NE = range(8)
STEPS = ((-1, 0), (1, 0), (0, -1), (0, 1), (-1, -1), (1, -1), (-1, 1), (1, 1))
OPPOSITE = (EAST, WEST, NORTH, SOUTH, NE, NW, SE, SW)


def rows_of(*rows):
    return jnp.concatenate(rows, axis=0)


def relaxed(east_dx, north_dx, east_dy, north_dy, stress, strength, ice):
    divergence = east_dx + north_dy
    tension = east_dx - north_dy
    shear = east_dy + north_dx
    inv = lax.rsqrt(divergence * divergence + 0.25 * (tension * tension + shear * shear) + DELTA_FLOOR)
    scaled = strength * inv
    return (
        (0.75 * stress[0] + 0.25 * (scaled * divergence - strength)) * ice,
        (0.75 * stress[1] + 0.0625 * (scaled * tension)) * ice,
        (0.75 * stress[2] + 0.03125 * (scaled * shear)) * ice,
    )


def drag_of(u, v, cu, cv):
    a = cu - u
    b = cv - v
    y = a * a + b * b + 0.01
    return y * lax.rsqrt(y)


def kernel(
    G, Y, R, C, B,
    vel_in, sig_in, mass_in, strength_in, mask_in, forcing_in,
    vel_out, sig_out, res_out, os_out,
    vel0, velb, sigb, mass, strength, ice, mask, forcing, ocean,
    pack, halo, turned,
    xs, xr, ys, yr, xs1, xr1, ys1, yr1, rs, rx, ry_s, ry,
    in_sem, f_send, f_recv, h_send, h_recv, i_send, i_recv, o_send, o_recv, r_send, r_recv, out_sem,
):
    gx = lax.axis_index("gx")
    gy = lax.axis_index("gy")

    def at(dx, dy):
        return {"gx": lax.rem(gx + dx + G, G), "gy": lax.rem(gy + dy + Y, Y)}

    inner = pl.ds(PAD, R)
    loads = [
        pltpu.make_async_copy(vel_in, velb.at[:, inner], in_sem.at[0]),
        pltpu.make_async_copy(sig_in, sigb.at[:, inner], in_sem.at[1]),
        pltpu.make_async_copy(strength_in, strength, in_sem.at[2]),
        pltpu.make_async_copy(mask_in, mask, in_sem.at[3]),
        pltpu.make_async_copy(vel_in, vel0, in_sem.at[4]),
        pltpu.make_async_copy(mass_in, mass, in_sem.at[5]),
    ]
    for copy in loads:
        copy.start()

    barrier = pltpu.get_barrier_semaphore()
    partners = [(d, 0) for d in range(1, G)] + [(0, d) for d in range(1, Y)] + list(STEPS[4:])
    for dx, dy in partners:
        pl.semaphore_signal(barrier, inc=1, device_id=at(dx, dy), device_id_type=MESH)
    pl.semaphore_wait(barrier, len(partners))

    mine = pl.ds(pl.multiple_of(gx * B, B), B)
    own_columns = pl.ds(pl.multiple_of(gx * C, C), C)
    own_forcing = pltpu.make_async_copy(forcing_in.at[:, :, own_columns], forcing.at[:, mine], f_recv.at[0])

    def send_forcing():
        sent = []
        for d in range(1, G):
            to = lax.rem(gx + d, G)
            copy = pltpu.make_async_remote_copy(
                src_ref=forcing_in.at[:, :, pl.ds(pl.multiple_of(to * C, C), C)],
                dst_ref=forcing.at[:, mine],
                send_sem=f_send.at[d],
                recv_sem=f_recv.at[d],
                device_id={"gx": to, "gy": gy},
                device_id_type=MESH,
            )
            copy.start()
            sent.append(copy)
        own_forcing.start()
        return sent

    def exchange(e):
        copies = []
        for n in range(8):
            src, dst = (xs.at[e], xr.at[e, n]) if n < 2 else (ys.at[e], yr.at[e, n - 2])
            slot = OPPOSITE[n]
            dst = xr.at[e, slot] if n < 2 else yr.at[e, slot - 2]
            copy = pltpu.make_async_remote_copy(
                src_ref=src, dst_ref=dst, send_sem=h_send.at[e, n], recv_sem=h_recv.at[e, slot],
                device_id=at(*STEPS[n]), device_id_type=MESH,
            )
            copy.start()
            copies.append(copy)
        return copies

    def arrive(e):
        for n in range(8):
            dst = xr.at[e, n] if n < 2 else yr.at[e, n - 2]
            pltpu.make_async_remote_copy(
                src_ref=dst, dst_ref=dst, send_sem=h_send.at[e, n], recv_sem=h_recv.at[e, n],
                device_id=at(*STEPS[n]), device_id_type=MESH,
            ).wait_recv()

    lanes = lax.broadcasted_iota(jnp.int32, (CH, C), 1)

    def pack_velocity(r0, u, v):
        pack[pl.ds(r0, CH), :] = jnp.where(
            lanes < 2, u,
            jnp.where(
                lanes < 4, pltpu.roll(v, 2, 1),
                jnp.where(lanes < 6, pltpu.roll(u, 6, 1), pltpu.roll(v, 8, 1)),
            ),
        )

    def chunks(body, init=0):
        def step(i, carry):
            return body(pl.multiple_of(i * CH, CH), carry)

        return lax.fori_loop(0, R // CH, step, init)

    def edge_rows(e):
        for q, (c, r) in enumerate(((0, 0), (0, 1), (1, 0), (1, 1), (0, R - 2), (0, R - 1), (1, R - 2), (1, R - 1))):
            ys[e, q : q + 1, :] = velb[c, PAD + r : PAD + r + 1, :]

    for copy in loads[:4]:
        copy.wait()

    def first_pack(r0, carry):
        rows = pl.ds(PAD + r0, CH)
        pack_velocity(r0, velb[0, rows, :], velb[1, rows, :])
        return carry

    chunks(first_pack)
    xs[0] = pack[...].T[0:8]
    edge_rows(0)
    started = exchange(0)

    def second_pack(r0, carry):
        rows = pl.ds(r0, CH)
        frac = mask[rows, :].astype(jnp.float32)
        ice[rows, :] = frac
        padded = pl.ds(PAD + r0, CH)
        fields = [sigb[0, padded, :], sigb[1, padded, :], sigb[2, padded, :], strength[rows, :], frac]
        out = jnp.zeros((CH, C), jnp.float32)
        for q, field in enumerate(fields):
            out = jnp.where(lanes == q, pltpu.roll(field, q, 1) if q else field, out)
            out = jnp.where(lanes == 8 + q, pltpu.roll(field, 9 + q, 1), out)
        pack[rows, :] = out
        return carry

    chunks(second_pack)
    xs1[...] = pack[...].T[0:16]
    ys1[...] = jnp.zeros_like(ys1)
    for q, r in ((0, 0), (8, R - 1)):
        for c in range(3):
            ys1[q + c : q + c + 1, :] = sigb[c, PAD + r : PAD + r + 1, :]
        ys1[q + 3 : q + 4, :] = strength[r : r + 1, :]
        ys1[q + 4 : q + 5, :] = ice[r : r + 1, :]
    fixed = []
    for n in range(4):
        slot = OPPOSITE[n]
        src, dst = (xs1, xr1.at[slot]) if n < 2 else (ys1, yr1.at[slot - 2])
        copy = pltpu.make_async_remote_copy(
            src_ref=src, dst_ref=dst, send_sem=i_send.at[n], recv_sem=i_recv.at[slot],
            device_id=at(*STEPS[n]), device_id_type=MESH,
        )
        copy.start()
        fixed.append(copy)
    sent_forcing = send_forcing()
    turned[...] = jnp.zeros_like(turned)

    has_south = (gy > 0).astype(jnp.float32)
    has_north = (gy < Y - 1).astype(jnp.float32)
    for copy in loads[4:]:
        copy.wait()
    for n in range(4):
        slot = OPPOSITE[n]
        dst = xr1.at[slot] if n < 2 else yr1.at[slot - 2]
        fixed[n].wait_recv()
    xw, xe, ysouth, ynorth = xr1[0], xr1[1], yr1[0], yr1[1]
    x_sig = [rows_of(xw[8 + c : 9 + c], xe[c : c + 1]) for c in range(3)]
    x_strength = rows_of(xw[11:12], xe[3:4])
    x_ice = rows_of(xw[12:13], xe[4:5])
    y_sig = [rows_of(ysouth[8 + c : 9 + c], ynorth[c : c + 1]) for c in range(3)]
    y_strength = rows_of(ysouth[11:12], ynorth[3:4])
    y_ice = rows_of(ysouth[12:13] * has_south, ynorth[4:5] * has_north)
    x_lane = lax.broadcasted_iota(jnp.int32, (4, R), 1)
    y_lane = lax.broadcasted_iota(jnp.int32, (4, C), 1)
    x_sign = jnp.where(lax.rem(lax.broadcasted_iota(jnp.int32, (4, R), 0), 2) == 0, 0.5, -0.5)
    y_sign = jnp.where(lax.rem(lax.broadcasted_iota(jnp.int32, (4, C), 0), 2) == 0, 0.5, -0.5)

    for k in range(ITERS):
        arrive(k)
        w, e = xr[k, 0], xr[k, 1]
        own = xs[k]
        s, n = yr[k, 0] * has_south, yr[k, 1] * has_north
        sw, se = yr[k, 2] * has_south, yr[k, 3] * has_south
        nw, ne = yr[k, 4] * has_north, yr[k, 5] * has_north
        own_y = ys[k]
        centre = rows_of(w[5:6], e[0:1], w[7:8], e[2:3])
        turned[0:4, :] = centre
        halo[...] = turned[...].T
        velb[0, PAD - 1 : PAD, :] = s[5:6]
        velb[1, PAD - 1 : PAD, :] = s[7:8]
        velb[0, PAD + R : PAD + R + 1, :] = n[0:1]
        velb[1, PAD + R : PAD + R + 1, :] = n[2:3]

        def sig_step(r0, carry):
            rows = pl.ds(r0, CH)
            mid = pl.ds(PAD + r0, CH)
            low = pl.ds(PAD - 1 + r0, CH)
            high = pl.ds(PAD + 1 + r0, CH)
            cols = halo[rows, :]
            slopes = []
            for c in range(2):
                f = velb[c, mid, :]
                right = jnp.where(lanes == C - 1, cols[:, 2 * c + 1 : 2 * c + 2], pltpu.roll(f, C - 1, 1))
                left = jnp.where(lanes == 0, cols[:, 2 * c : 2 * c + 1], pltpu.roll(f, 1, 1))
                slopes.append(0.5 * (right - left))
            for c in range(2):
                slopes.append(0.5 * (velb[c, high, :] - velb[c, low, :]))
            new = relaxed(
                slopes[0], slopes[1], slopes[2], slopes[3],
                [sigb[c, mid, :] for c in range(3)], strength[rows, :], ice[rows, :],
            )
            for c in range(3):
                sigb[c, mid, :] = new[c]
            return carry

        chunks(sig_step)

        x_dx = x_sign * (rows_of(own[0:1], own[5:6], own[2:3], own[7:8]) - rows_of(w[4:5], e[1:2], w[6:7], e[3:4]))

        def corner(a, b, q, lane_a, lane_b, length):
            parts = []
            for ref, row, lane in ((a, q[0], lane_a), (b, q[1], lane_b), (a, q[2], lane_a), (b, q[3], lane_b)):
                parts.append(jnp.broadcast_to(ref[row : row + 1, lane : lane + 1], (1, length)))
            return rows_of(*parts)

        below = jnp.where(x_lane == 0, corner(sw, se, (5, 5, 7, 7), C - 1, 0, R), pltpu.roll(centre, 1, 1))
        above = jnp.where(x_lane == R - 1, corner(nw, ne, (0, 0, 2, 2), C - 1, 0, R), pltpu.roll(centre, R - 1, 1))
        x_dy = 0.5 * (above - below)
        x_sig = relaxed(x_dx[0:2], x_dx[2:4], x_dy[0:2], x_dy[2:4], x_sig, x_strength, x_ice)

        centre_y = rows_of(s[5:6], n[0:1], s[7:8], n[2:3])
        y_dy = y_sign * (
            rows_of(own_y[0:1], own_y[5:6], own_y[2:3], own_y[7:8]) - rows_of(s[4:5], n[1:2], s[6:7], n[3:4])
        )
        left = jnp.where(y_lane == 0, corner(sw, nw, (5, 0, 7, 2), C - 1, C - 1, C), pltpu.roll(centre_y, 1, 1))
        right = jnp.where(y_lane == C - 1, corner(se, ne, (5, 0, 7, 2), 0, 0, C), pltpu.roll(centre_y, C - 1, 1))
        y_dx = 0.5 * (right - left)
        y_sig = relaxed(y_dx[0:2], y_dx[2:4], y_dy[0:2], y_dy[2:4], y_sig, y_strength, y_ice)
        for c in range(3):
            sigb[c, PAD - 1 : PAD, :] = y_sig[c][0:1]
            sigb[c, PAD + R : PAD + R + 1, :] = y_sig[c][1:2]
        turned[0:4, :] = rows_of(0.5 * (x_sig[0] + x_sig[1]), x_sig[2])
        halo[...] = turned[...].T
        if k == ITERS - 1:
            keep_sig = pltpu.make_async_copy(sigb.at[:, inner], sig_out, out_sem.at[0])
            keep_sig.start()

        if k == 0:
            own_forcing.wait()
            for copy in sent_forcing:
                copy.wait_recv()

        last = k == ITERS - 1

        def vel_step(r0, total):
            rows = pl.ds(r0, CH)
            mid = pl.ds(PAD + r0, CH)
            low = pl.ds(PAD - 1 + r0, CH)
            high = pl.ds(PAD + 1 + r0, CH)
            cols = halo[rows, :]
            sxx = 0.5 * (sigb[0, mid, :] + sigb[1, mid, :])
            sxy = sigb[2, mid, :]

            def dx(f, q):
                right = jnp.where(lanes == C - 1, cols[:, q + 1 : q + 2], pltpu.roll(f, C - 1, 1))
                left = jnp.where(lanes == 0, cols[:, q : q + 1], pltpu.roll(f, 1, 1))
                return 0.5 * (right - left)

            dy_xy = 0.5 * (sigb[2, high, :] - sigb[2, low, :])
            dy_yy = 0.25 * ((sigb[0, high, :] - sigb[1, high, :]) - (sigb[0, low, :] - sigb[1, low, :]))
            force_east = dx(sxx, 0) + dy_xy
            force_north = dx(sxy, 2) + dy_yy
            u = velb[0, mid, :]
            v = velb[1, mid, :]
            cu = forcing[2, rows, :]
            cv = forcing[3, rows, :]
            frac = ice[rows, :]
            drag = drag_of(u, v, cu, cv)
            if k == 0:
                inv_mass = 1.0 / mass[rows, :]
                mass[rows, :] = inv_mass
            else:
                inv_mass = mass[rows, :]
            inv_den = frac / (5.0 + drag * inv_mass)
            lat = (gy * R + r0 + lax.broadcasted_iota(jnp.int32, (CH, C), 0)).astype(jnp.float32)
            coriolis = 0.3 + 1.2 * (lat + 0.5) / (R * Y)
            new_u = (
                4.0 * u + vel0[0, rows, :] + (force_east + forcing[0, rows, :] + drag * cu) * inv_mass + coriolis * v
            ) * inv_den
            new_v = (
                4.0 * v + vel0[1, rows, :] + (force_north + forcing[1, rows, :] + drag * cv) * inv_mass - coriolis * u
            ) * inv_den
            velb[0, mid, :] = new_u
            velb[1, mid, :] = new_v
            if last:
                final = drag_of(new_u, new_v, cu, cv) * frac
                ocean[0, rows, :] = final * (new_u - cu)
                ocean[1, rows, :] = final * (new_v - cv)
            else:
                pack_velocity(r0, new_u, new_v)
            du = new_u - u
            dv = new_v - v
            return total + du * du + dv * dv

        total = chunks(vel_step, jnp.zeros((CH, C), jnp.float32))
        if not last:
            edge_rows(k + 1)
            xs[k + 1] = pack[...].T[0:8]
            started += exchange(k + 1)
        rs[k : k + 1, :] = jnp.sum(total, axis=0, keepdims=True)

    rs[ITERS:8, :] = jnp.zeros((8 - ITERS, C), jnp.float32)
    sums = []
    for d in range(1, G):
        copy = pltpu.make_async_remote_copy(
            src_ref=rs, dst_ref=rx.at[gx], send_sem=r_send.at[d], recv_sem=r_recv.at[d],
            device_id=at(d, 0), device_id_type=MESH,
        )
        copy.start()
        sums.append(copy)
    outs = []
    for d in range(1, G):
        to = lax.rem(gx + d, G)
        copy = pltpu.make_async_remote_copy(
            src_ref=ocean.at[:, pl.ds(pl.multiple_of(to * B, B), B)],
            dst_ref=os_out.at[:, :, own_columns],
            send_sem=o_send.at[d], recv_sem=o_recv.at[d],
            device_id={"gx": to, "gy": gy}, device_id_type=MESH,
        )
        copy.start()
        outs.append(copy)
    own_out = pltpu.make_async_copy(ocean.at[:, mine], os_out.at[:, :, own_columns], out_sem.at[1])
    own_out.start()
    keep_vel = pltpu.make_async_copy(velb.at[:, inner], vel_out, out_sem.at[2])
    keep_vel.start()
    for copy in sums:
        copy.wait_recv()
    rx[gx] = rs[...]
    total = rx[0]
    for d in range(1, G):
        total = total + rx[d]
    ry_s[...] = total
    ry[gy] = total
    for d in range(1, Y):
        copy = pltpu.make_async_remote_copy(
            src_ref=ry_s, dst_ref=ry.at[gy], send_sem=r_send.at[G + d], recv_sem=r_recv.at[G + d],
            device_id=at(0, d), device_id_type=MESH,
        )
        copy.start()
        sums.append(copy)
    for copy in sums[G - 1 :]:
        copy.wait_recv()
    total = ry[0]
    for d in range(1, Y):
        total = total + ry[d]
    for k in range(ITERS):
        res_out[k] = jnp.sum(total[k : k + 1])
    for copy in outs:
        copy.wait_recv()
    for copy in started + fixed + sent_forcing + outs + sums:
        copy.wait_send()
    own_out.wait()
    keep_vel.wait()
    keep_sig.wait()


def local(velocity, stress, ice_mass, strength, land_mask, ocean_forcing):
    G, Y = lax.axis_size("gx"), lax.axis_size("gy")
    R, C = velocity.shape[1:]
    B = ocean_forcing.shape[1]
    f32 = jnp.float32
    dma = pltpu.SemaphoreType.DMA
    any_space = pl.BlockSpec(memory_space=pl.ANY)
    return pl.pallas_call(
        functools.partial(kernel, G, Y, R, C, B),
        out_shape=(
            jax.ShapeDtypeStruct(velocity.shape, f32),
            jax.ShapeDtypeStruct(stress.shape, f32),
            jax.ShapeDtypeStruct((ITERS,), f32),
            jax.ShapeDtypeStruct((2,) + ocean_forcing.shape[1:], f32),
        ),
        in_specs=[any_space] * 6,
        out_specs=(any_space, any_space, pl.BlockSpec(memory_space=pltpu.SMEM), any_space),
        scratch_shapes=[
            pltpu.VMEM((2, R, C), f32),
            pltpu.VMEM((2, R + 2 * PAD, C), f32),
            pltpu.VMEM((3, R + 2 * PAD, C), f32),
            pltpu.VMEM((R, C), f32),
            pltpu.VMEM((R, C), f32),
            pltpu.VMEM((R, C), f32),
            pltpu.VMEM((R, C), jnp.int32),
            pltpu.VMEM((4, R, C), f32),
            pltpu.VMEM((2, R, C), f32),
            pltpu.VMEM((R, C), f32),
            pltpu.VMEM((R, C), f32),
            pltpu.VMEM((C, R), f32),
            pltpu.VMEM((ITERS, 8, R), f32),
            pltpu.VMEM((ITERS, 2, 8, R), f32),
            pltpu.VMEM((ITERS, 8, C), f32),
            pltpu.VMEM((ITERS, 6, 8, C), f32),
            pltpu.VMEM((16, R), f32),
            pltpu.VMEM((2, 16, R), f32),
            pltpu.VMEM((16, C), f32),
            pltpu.VMEM((2, 16, C), f32),
            pltpu.VMEM((8, C), f32),
            pltpu.VMEM((G, 8, C), f32),
            pltpu.VMEM((8, C), f32),
            pltpu.VMEM((Y, 8, C), f32),
            dma((6,)),
            dma((G,)),
            dma((G,)),
            dma((ITERS, 8)),
            dma((ITERS, 8)),
            dma((4,)),
            dma((4,)),
            dma((G,)),
            dma((G,)),
            dma((G + Y,)),
            dma((G + Y,)),
            dma((3,)),
        ],
        compiler_params=pltpu.CompilerParams(collective_id=0, has_side_effects=True),
    )(velocity, stress, ice_mass, strength, land_mask, ocean_forcing)


def solution(mesh):
    placed = (
        P(None, "gy", "gx"),
        P(None, "gy", "gx"),
        P("gy", "gx"),
        P("gy", "gx"),
        P("gy", "gx"),
        P(None, ("gy", "gx"), None),
    )
    return jax.shard_map(
        local,
        mesh=mesh,
        in_specs=placed,
        out_specs=(P(None, "gy", "gx"), P(None, "gy", "gx"), P(), P(None, ("gy", "gx"), None)),
        check_vma=False,
    )
```

```python
import functools

import jax
import jax.numpy as jnp
from jax import lax
from jax.experimental import pallas as pl
from jax.experimental.pallas import tpu as pltpu
from jax.sharding import PartitionSpec as P

ITERS = 4
DELTA_FLOOR = 0.0025
DEEP = 8
PAD = 16
SIDE = 128
MESH = pl.DeviceIdType.MESH

WEST, EAST, SOUTH, NORTH, SW, SE, NW, NE = range(8)
STEPS = ((-1, 0), (1, 0), (0, -1), (0, 1), (-1, -1), (1, -1), (-1, 1), (1, 1))
OPPOSITE = (EAST, WEST, NORTH, SOUTH, NE, NW, SE, SW)


def rows_of(*rows):
    return jnp.concatenate(rows, axis=0)


def relaxed(east_dx, north_dx, east_dy, north_dy, stress, strength, ice):
    divergence = east_dx + north_dy
    tension = east_dx - north_dy
    shear = east_dy + north_dx
    inv = lax.rsqrt(divergence * divergence + 0.25 * (tension * tension + shear * shear) + DELTA_FLOOR)
    scaled = strength * inv
    return (
        (0.75 * stress[0] + 0.25 * (scaled * divergence - strength)) * ice,
        (0.75 * stress[1] + 0.0625 * (scaled * tension)) * ice,
        (0.75 * stress[2] + 0.03125 * (scaled * shear)) * ice,
    )


def drag_of(u, v, cu, cv):
    a = cu - u
    b = cv - v
    y = a * a + b * b + 0.01
    return y * lax.rsqrt(y)


def moved(u, v, start, force_east, force_north, fe, fn, cu, cv, inv_mass, coriolis, frac):
    drag = drag_of(u, v, cu, cv)
    inv_den = frac / (5.0 + drag * inv_mass)
    new_u = (4.0 * u + start[0] + (force_east + fe + drag * cu) * inv_mass + coriolis * v) * inv_den
    new_v = (4.0 * v + start[1] + (force_north + fn + drag * cv) * inv_mass - coriolis * u) * inv_den
    return new_u, new_v


def kernel(
    G, Y, R, C, B,
    vel_in, sig_in, mass_in, strength_in, mask_in, forcing_in,
    vel_out, sig_out, res_out, os_out,
    vel0, velb, sigb, mass, strength, ice, mask, bands, forcing, ocean,
    pack, halo, turned, low, high, strip, f_out, f_in, f_strip,
    rs, rx, ry_s, ry,
    in_sem, f_send, f_recv, s_send, s_recv, e_send, e_recv, h_send, h_recv, y_send, y_recv,
    o_send, o_recv, r_send, r_recv, out_sem,
):
    gx = lax.axis_index("gx")
    gy = lax.axis_index("gy")
    L = R + 2 * SIDE
    SHIFT = SIDE - PAD

    def at(dx, dy):
        return {"gx": lax.rem(gx + dx + G, G), "gy": lax.rem(gy + dy + Y, Y)}

    def remote(src, dst, send, recv, where):
        return pltpu.make_async_remote_copy(
            src_ref=src, dst_ref=dst, send_sem=send, recv_sem=recv, device_id=where, device_id_type=MESH
        )

    inner = pl.ds(PAD, R)
    loads = [
        pltpu.make_async_copy(vel_in, velb.at[:, inner], in_sem.at[0]),
        pltpu.make_async_copy(sig_in, sigb.at[:, inner], in_sem.at[1]),
        pltpu.make_async_copy(mass_in, mass.at[inner], in_sem.at[2]),
        pltpu.make_async_copy(strength_in, strength.at[inner], in_sem.at[3]),
        pltpu.make_async_copy(mask_in, mask.at[inner], in_sem.at[4]),
        pltpu.make_async_copy(forcing_in, bands, in_sem.at[5]),
    ]
    for copy in loads:
        copy.start()

    barrier = pltpu.get_barrier_semaphore()
    partners = [(dx, dy) for dy in range(Y) for dx in range(G) if (dx or dy) and (dx == 0 or dy in (0, 1, Y - 1))]
    for dx, dy in partners:
        pl.semaphore_signal(barrier, inc=1, device_id=at(dx, dy), device_id_type=MESH)

    for ref in (velb, sigb, forcing):
        for c in range(ref.shape[0]):
            for r in (0, PAD + R + DEEP):
                ref[c, r : r + DEEP, :] = jnp.zeros((DEEP, C), jnp.float32)
    for ref in (turned, pack, f_strip, f_out):
        ref[...] = jnp.zeros_like(ref)

    for copy in loads[:5]:
        copy.wait()
    fields = [velb.at[0], velb.at[1], sigb.at[0], sigb.at[1], sigb.at[2], mass, strength, mask]
    for q, field in enumerate(fields):
        t = field[PAD : PAD + R, :].astype(jnp.float32).T
        low[q] = t[0:DEEP]
        high[q] = t[C - DEEP : C]
    loads[5].wait()
    for c in range(G):
        t = bands[:, :, c * C : (c + 1) * C].reshape(4 * B, C).T
        f_out[(c + 1) % G, 0:DEEP, 0 : 4 * B] = t[C - DEEP : C]
        f_out[(c + G - 1) % G, DEEP : 2 * DEEP, 0 : 4 * B] = t[0:DEEP]
    f_in[gx] = f_out[gx]

    pl.semaphore_wait(barrier, len(partners))

    near, far = pl.ds(0, DEEP), pl.ds(DEEP, DEEP)
    centre, before, after = pl.ds(SIDE, R), pl.ds(0, SIDE), pl.ds(SIDE + R, SIDE)
    first, final_rows = pl.ds(0, SIDE), pl.ds(R - SIDE, SIDE)
    plan = (
        (WEST, low, strip.at[:, far, centre]),
        (EAST, high, strip.at[:, near, centre]),
        (SW, low.at[:, :, first], strip.at[:, far, after]),
        (SE, high.at[:, :, first], strip.at[:, near, after]),
        (NW, low.at[:, :, final_rows], strip.at[:, far, before]),
        (NE, high.at[:, :, final_rows], strip.at[:, near, before]),
    )
    started = []
    for n, (way, src, dst) in enumerate(plan):
        started.append(remote(src, dst, h_send.at[n], h_recv.at[n], at(*STEPS[way])))
    bottom, top = pl.ds(PAD, DEEP), pl.ds(PAD + R - DEEP, DEEP)
    under, over = pl.ds(PAD - DEEP, DEEP), pl.ds(PAD + R, DEEP)
    for n, ref in enumerate((velb, sigb, mass, strength, mask)):
        for m, (way, src, dst) in enumerate(((SOUTH, bottom, over), (NORTH, top, under))):
            a, b = (ref.at[:, src], ref.at[:, dst]) if len(ref.shape) == 3 else (ref.at[src], ref.at[dst])
            started.append(remote(a, b, y_send.at[2 * n + m], y_recv.at[2 * n + m], at(*STEPS[way])))

    mine = pl.ds(pl.multiple_of(gx * B, B), B)
    padded_mine = pl.ds(pl.multiple_of(PAD + gx * B, DEEP), B)
    own_columns = pl.ds(pl.multiple_of(gx * C, C), C)
    own_forcing = pltpu.make_async_copy(bands.at[:, :, own_columns], forcing.at[:, padded_mine], f_recv.at[0])
    for d in range(1, G):
        to = lax.rem(gx + d, G)
        columns = pl.ds(pl.multiple_of(to * C, C), C)
        started.append(remote(bands.at[:, :, columns], forcing.at[:, padded_mine], f_send.at[d], f_recv.at[d], at(d, 0)))
        started.append(remote(f_out.at[to], f_in.at[gx], s_send.at[d], s_recv.at[d], at(d, 0)))
    for copy in started:
        copy.start()
    own_forcing.start()

    def beyond(side):
        step, src, dst = ((1, pl.ds(B - DEEP, DEEP), under), (-1, near, over))[side]
        copies = []
        for d in range(G):
            where = {"gx": d, "gy": lax.rem(gy + step + Y, Y)}
            k = 2 * side
            copies.append(
                remote(bands.at[:, src, pl.ds(d * C, C)], forcing.at[:, dst], e_send.at[d, k], e_recv.at[k], where)
            )
            copies.append(remote(f_out.at[d], f_in.at[G + side], e_send.at[d, k + 1], e_recv.at[k + 1], where))
        return copies

    edges = ((G - 1, 0), (0, 1))
    for holder, side in edges:

        @pl.when(gx == holder)
        def _():
            for copy in beyond(side):
                copy.start()

    for copy in started[:16]:
        copy.wait_recv()
    for copy in started[6:16]:
        copy.wait_send()

    has_south = (gy > 0).astype(jnp.float32)
    has_north = (gy < Y - 1).astype(jnp.float32)
    for c in range(2):
        velb[c, under, :] = velb[c, under, :] * has_south
        velb[c, over, :] = velb[c, over, :] * has_north
    ice[...] = mask[...].astype(jnp.float32)
    ice[under, :] = ice[under, :] * has_south
    ice[over, :] = ice[over, :] * has_north
    for c in range(2):
        vel0[c] = velb[c, PAD - DEEP : PAD + R + DEEP, :]

    strip_lane = lax.broadcasted_iota(jnp.int32, (2 * DEEP, L), 1)
    strip_row = lax.broadcasted_iota(jnp.int32, (2 * DEEP, L), 0)
    lat_s = strip_lane - SIDE + gy * R
    inside = ((lat_s >= 0) & (lat_s < R * Y)).astype(jnp.float32)
    cor_s = 0.3 + 1.2 * (lat_s.astype(jnp.float32) + 0.5) / (R * Y)
    sv = [strip[0] * inside, strip[1] * inside]
    sv0 = list(sv)
    ss = [strip[2], strip[3], strip[4]]
    s_strength = strip[6]
    s_ice = strip[7] * inside
    s_inv_mass = 1.0 / strip[5]

    def strip_dx(f, lo, hi):
        right = jnp.where(strip_row == DEEP - 1, lo, pltpu.roll(f, 2 * DEEP - 1, 0))
        left = jnp.where(strip_row == DEEP, hi, pltpu.roll(f, 1, 0))
        return 0.5 * (right - left)

    def strip_dy(f):
        return 0.5 * (pltpu.roll(f, L - 1, 1) - pltpu.roll(f, 1, 1))

    pieces = ((PAD - DEEP, DEEP), (PAD + R, DEEP)) + tuple((PAD + r, R // 2) for r in range(0, R, R // 2))

    def lane_of(n):
        return lax.broadcasted_iota(jnp.int32, (n, C), 1)

    def pack_pair(p, n, a, b):
        lane = lane_of(n)
        pack[p + SHIFT : p + SHIFT + n, :] = jnp.where(
            lane < 1, a, jnp.where(lane < 2, pltpu.roll(a, 2, 1), jnp.where(lane < 3, pltpu.roll(b, 2, 1), pltpu.roll(b, 4, 1)))
        )

    def ring(a, b):
        turned[0:2, :] = a[DEEP - 1 : DEEP + 1]
        turned[2:4, :] = b[DEEP - 1 : DEEP + 1]
        halo[...] = turned[...].T

    def main_dx(f, cols, q, lane):
        right = jnp.where(lane == C - 1, cols[:, q + 1 : q + 2], pltpu.roll(f, C - 1, 1))
        left = jnp.where(lane == 0, cols[:, q : q + 1], pltpu.roll(f, 1, 1))
        return 0.5 * (right - left)

    for p, n in pieces:
        pack_pair(p, n, velb[0, p : p + n, :], velb[1, p : p + n, :])

    for k in range(ITERS):
        last = k == ITERS - 1
        edge = pack[...].T[0:8]
        ring(sv[0], sv[1])
        for p, n in pieces:
            lane = lane_of(n)
            cols = halo[p + SHIFT : p + SHIFT + n, :]
            slopes = [main_dx(velb[c, p : p + n, :], cols, 2 * c, lane) for c in range(2)]
            slopes += [0.5 * (velb[c, p + 1 : p + n + 1, :] - velb[c, p - 1 : p + n - 1, :]) for c in range(2)]
            new = relaxed(
                *slopes, [sigb[c, p : p + n, :] for c in range(3)], strength[p : p + n, :], ice[p : p + n, :]
            )
            for c in range(3):
                sigb[c, p : p + n, :] = new[c]
            pack_pair(p, n, 0.5 * (new[0] + new[1]), new[2])
        if last:
            keep_sig = pltpu.make_async_copy(sigb.at[:, inner], sig_out, out_sem.at[0])
            keep_sig.start()
        ss = relaxed(
            strip_dx(sv[0], edge[0:1], edge[1:2]), strip_dx(sv[1], edge[2:3], edge[3:4]),
            strip_dy(sv[0]), strip_dy(sv[1]), ss, s_strength, s_ice,
        )
        s_xx = 0.5 * (ss[0] + ss[1])
        edge = pack[...].T[0:8]
        ring(s_xx, ss[2])

        if k == 0:
            own_forcing.wait()
            for copy in started[16:]:
                copy.wait_recv()
            for side in range(2):
                for copy, slot in ((0, forcing.at[:, (under, over)[side]]), (1, f_in.at[G + side])):
                    m = 2 * side + copy
                    remote(slot, slot, e_send.at[0, m], e_recv.at[m], at(0, 1)).wait_recv()
            for f in range(4):
                for b in range(-1, G + 1):
                    slot = G if b < 0 else G + 1 if b == G else b
                    a = SIDE + b * B
                    f_strip[f, :, a : a + B] = f_in[slot, :, f * B : (f + 1) * B]

        total = jnp.zeros((R // 2, C), jnp.float32)
        for p, n in pieces:
            if last and n == DEEP:
                continue
            lane = lane_of(n)
            cols = halo[p + SHIFT : p + SHIFT + n, :]
            sxx = 0.5 * (sigb[0, p : p + n, :] + sigb[1, p : p + n, :])
            sxy = sigb[2, p : p + n, :]
            hi, lo = pl.ds(p + 1, n), pl.ds(p - 1, n)
            dy_xy = 0.5 * (sigb[2, hi, :] - sigb[2, lo, :])
            dy_yy = 0.25 * ((sigb[0, hi, :] - sigb[1, hi, :]) - (sigb[0, lo, :] - sigb[1, lo, :]))
            force_east = main_dx(sxx, cols, 0, lane) + dy_xy
            force_north = main_dx(sxy, cols, 2, lane) + dy_yy
            u, v = velb[0, p : p + n, :], velb[1, p : p + n, :]
            fe, fn, cu, cv = (forcing[c, p : p + n, :] for c in range(4))
            frac = ice[p : p + n, :]
            if k == 0:
                inv_mass = 1.0 / mass[p : p + n, :]
                mass[p : p + n, :] = inv_mass
            else:
                inv_mass = mass[p : p + n, :]
            lat = (gy * R + (p - PAD) + lax.broadcasted_iota(jnp.int32, (n, C), 0)).astype(jnp.float32)
            coriolis = 0.3 + 1.2 * (lat + 0.5) / (R * Y)
            start = [vel0[c, p - PAD + DEEP : p - PAD + DEEP + n, :] for c in range(2)]
            new_u, new_v = moved(u, v, start, force_east, force_north, fe, fn, cu, cv, inv_mass, coriolis, frac)
            velb[0, p : p + n, :] = new_u
            velb[1, p : p + n, :] = new_v
            if last:
                drag = drag_of(new_u, new_v, cu, cv) * frac
                ocean[0, p - PAD : p - PAD + n, :] = drag * (new_u - cu)
                ocean[1, p - PAD : p - PAD + n, :] = drag * (new_v - cv)
            else:
                pack_pair(p, n, new_u, new_v)
            if n > DEEP:
                du = new_u - u
                dv = new_v - v
                total = total + (du * du + dv * dv)
        rs[k : k + 1, :] = jnp.sum(total, axis=0, keepdims=True)
        if not last:
            s_yy = 0.5 * (ss[0] - ss[1])
            force_east = strip_dx(s_xx, edge[0:1], edge[1:2]) + strip_dy(ss[2])
            force_north = strip_dx(ss[2], edge[2:3], edge[3:4]) + strip_dy(s_yy)
            sv = list(
                moved(
                    sv[0], sv[1], sv0, force_east, force_north,
                    f_strip[0], f_strip[1], f_strip[2], f_strip[3], s_inv_mass, cor_s, s_ice,
                )
            )

    rs[ITERS:8, :] = jnp.zeros((8 - ITERS, C), jnp.float32)
    sums = []
    for d in range(1, G):
        copy = pltpu.make_async_remote_copy(
            src_ref=rs, dst_ref=rx.at[gx], send_sem=r_send.at[d], recv_sem=r_recv.at[d],
            device_id=at(d, 0), device_id_type=MESH,
        )
        copy.start()
        sums.append(copy)
    outs = []
    for d in range(1, G):
        to = lax.rem(gx + d, G)
        copy = pltpu.make_async_remote_copy(
            src_ref=ocean.at[:, pl.ds(pl.multiple_of(to * B, B), B)],
            dst_ref=os_out.at[:, :, own_columns],
            send_sem=o_send.at[d], recv_sem=o_recv.at[d],
            device_id={"gx": to, "gy": gy}, device_id_type=MESH,
        )
        copy.start()
        outs.append(copy)
    own_out = pltpu.make_async_copy(ocean.at[:, mine], os_out.at[:, :, own_columns], out_sem.at[1])
    own_out.start()
    keep_vel = pltpu.make_async_copy(velb.at[:, inner], vel_out, out_sem.at[2])
    keep_vel.start()
    for copy in sums:
        copy.wait_recv()
    rx[gx] = rs[...]
    total = rx[0]
    for d in range(1, G):
        total = total + rx[d]
    ry_s[...] = total
    ry[gy] = total
    for d in range(1, Y):
        copy = pltpu.make_async_remote_copy(
            src_ref=ry_s, dst_ref=ry.at[gy], send_sem=r_send.at[G + d], recv_sem=r_recv.at[G + d],
            device_id=at(0, d), device_id_type=MESH,
        )
        copy.start()
        sums.append(copy)
    for copy in sums[G - 1 :]:
        copy.wait_recv()
    total = ry[0]
    for d in range(1, Y):
        total = total + ry[d]
    for k in range(ITERS):
        res_out[k] = jnp.sum(total[k : k + 1])
    for copy in outs:
        copy.wait_recv()
    for copy in started[:6] + started[16:] + outs + sums:
        copy.wait_send()
    for holder, side in edges:

        @pl.when(gx == holder)
        def _():
            for copy in beyond(side):
                copy.wait_send()

    own_out.wait()
    keep_vel.wait()
    keep_sig.wait()


def local(velocity, stress, ice_mass, strength, land_mask, ocean_forcing):
    G, Y = lax.axis_size("gx"), lax.axis_size("gy")
    R, C = velocity.shape[1:]
    B = ocean_forcing.shape[1]
    L = R + 2 * SIDE
    f32 = jnp.float32
    dma = pltpu.SemaphoreType.DMA
    any_space = pl.BlockSpec(memory_space=pl.ANY)
    return pl.pallas_call(
        functools.partial(kernel, G, Y, R, C, B),
        out_shape=(
            jax.ShapeDtypeStruct(velocity.shape, f32),
            jax.ShapeDtypeStruct(stress.shape, f32),
            jax.ShapeDtypeStruct((ITERS,), f32),
            jax.ShapeDtypeStruct((2,) + ocean_forcing.shape[1:], f32),
        ),
        in_specs=[any_space] * 6,
        out_specs=(any_space, any_space, pl.BlockSpec(memory_space=pltpu.SMEM), any_space),
        scratch_shapes=[
            pltpu.VMEM((2, R + 2 * DEEP, C), f32),
            pltpu.VMEM((2, R + 2 * PAD, C), f32),
            pltpu.VMEM((3, R + 2 * PAD, C), f32),
            pltpu.VMEM((R + 2 * PAD, C), f32),
            pltpu.VMEM((R + 2 * PAD, C), f32),
            pltpu.VMEM((R + 2 * PAD, C), f32),
            pltpu.VMEM((R + 2 * PAD, C), jnp.int32),
            pltpu.VMEM(ocean_forcing.shape, f32),
            pltpu.VMEM((4, R + 2 * PAD, C), f32),
            pltpu.VMEM((2, R, C), f32),
            pltpu.VMEM((L, C), f32),
            pltpu.VMEM((L, C), f32),
            pltpu.VMEM((C, L), f32),
            pltpu.VMEM((8, DEEP, R), f32),
            pltpu.VMEM((8, DEEP, R), f32),
            pltpu.VMEM((8, 2 * DEEP, L), f32),
            pltpu.VMEM((G, 2 * DEEP, SIDE), f32),
            pltpu.VMEM((G + 2, 2 * DEEP, SIDE), f32),
            pltpu.VMEM((4, 2 * DEEP, L), f32),
            pltpu.VMEM((8, C), f32),
            pltpu.VMEM((G, 8, C), f32),
            pltpu.VMEM((8, C), f32),
            pltpu.VMEM((Y, 8, C), f32),
            dma((6,)),
            dma((G,)),
            dma((G,)),
            dma((G,)),
            dma((G,)),
            dma((G, 4)),
            dma((4,)),
            dma((6,)),
            dma((6,)),
            dma((10,)),
            dma((10,)),
            dma((G,)),
            dma((G,)),
            dma((G + Y,)),
            dma((G + Y,)),
            dma((3,)),
        ],
        compiler_params=pltpu.CompilerParams(collective_id=0, has_side_effects=True),
    )(velocity, stress, ice_mass, strength, land_mask, ocean_forcing)


def solution(mesh):
    placed = (
        P(None, "gy", "gx"),
        P(None, "gy", "gx"),
        P("gy", "gx"),
        P("gy", "gx"),
        P("gy", "gx"),
        P(None, ("gy", "gx"), None),
    )
    return jax.shard_map(
        local,
        mesh=mesh,
        in_specs=placed,
        out_specs=(P(None, "gy", "gx"), P(None, "gy", "gx"), P(), P(None, ("gy", "gx"), None)),
        check_vma=False,
    )
```

```python
import functools

import jax
import jax.numpy as jnp
from jax import lax
from jax.experimental import pallas as pl
from jax.experimental.pallas import tpu as pltpu
from jax.sharding import PartitionSpec as P

ITERS = 4
DELTA_FLOOR = 0.0025
DEEP = 8
PAD = 16
SIDE = 128
MESH = pl.DeviceIdType.MESH

WEST, EAST, SOUTH, NORTH, SW, SE, NW, NE = range(8)
STEPS = ((-1, 0), (1, 0), (0, -1), (0, 1), (-1, -1), (1, -1), (-1, 1), (1, 1))
OPPOSITE = (EAST, WEST, NORTH, SOUTH, NE, NW, SE, SW)


def rows_of(*rows):
    return jnp.concatenate(rows, axis=0)


def relaxed(east_dx, north_dx, east_dy, north_dy, stress, strength, ice):
    divergence = east_dx + north_dy
    tension = east_dx - north_dy
    shear = east_dy + north_dx
    inv = lax.rsqrt(divergence * divergence + 0.25 * (tension * tension + shear * shear) + DELTA_FLOOR)
    scaled = strength * inv
    return (
        (0.75 * stress[0] + 0.25 * (scaled * divergence - strength)) * ice,
        (0.75 * stress[1] + 0.0625 * (scaled * tension)) * ice,
        (0.75 * stress[2] + 0.03125 * (scaled * shear)) * ice,
    )


def drag_of(u, v, cu, cv):
    a = cu - u
    b = cv - v
    y = a * a + b * b + 0.01
    return y * lax.rsqrt(y)


def moved(u, v, start, force_east, force_north, fe, fn, cu, cv, inv_mass, coriolis, frac):
    drag = drag_of(u, v, cu, cv)
    inv_den = frac / (5.0 + drag * inv_mass)
    new_u = (4.0 * u + start[0] + (force_east + fe + drag * cu) * inv_mass + coriolis * v) * inv_den
    new_v = (4.0 * v + start[1] + (force_north + fn + drag * cv) * inv_mass - coriolis * u) * inv_den
    return new_u, new_v


def kernel(
    G, Y, R, C, B,
    vel_in, sig_in, mass_in, strength_in, mask_in, forcing_in,
    vel_out, sig_out, res_out, os_out,
    vel0, velb, sigb, mass, strength, ice, mask, bands, forcing, ocean,
    pack, halo, turned, low, high, strip, f_out, f_in, f_strip,
    rs, rx,
    in_sem, f_send, f_recv, s_send, s_recv, e_send, e_recv, h_send, h_recv, y_send, y_recv,
    o_send, o_recv, r_send, r_recv, out_sem,
):
    gx = lax.axis_index("gx")
    gy = lax.axis_index("gy")
    L = R + 2 * SIDE
    SHIFT = SIDE - PAD

    def at(dx, dy):
        return {"gx": lax.rem(gx + dx + G, G), "gy": lax.rem(gy + dy + Y, Y)}

    def remote(src, dst, send, recv, where):
        return pltpu.make_async_remote_copy(
            src_ref=src, dst_ref=dst, send_sem=send, recv_sem=recv, device_id=where, device_id_type=MESH
        )

    inner = pl.ds(PAD, R)
    loads = [
        pltpu.make_async_copy(vel_in, velb.at[:, inner], in_sem.at[0]),
        pltpu.make_async_copy(sig_in, sigb.at[:, inner], in_sem.at[1]),
        pltpu.make_async_copy(mass_in, mass.at[inner], in_sem.at[2]),
        pltpu.make_async_copy(strength_in, strength.at[inner], in_sem.at[3]),
        pltpu.make_async_copy(mask_in, mask.at[inner], in_sem.at[4]),
        pltpu.make_async_copy(forcing_in, bands, in_sem.at[5]),
    ]
    for copy in loads:
        copy.start()

    barrier = pltpu.get_barrier_semaphore()
    partners = [(dx, dy) for dy in range(Y) for dx in range(G) if dx or dy]
    for dx, dy in partners:
        pl.semaphore_signal(barrier, inc=1, device_id=at(dx, dy), device_id_type=MESH)

    for ref in (velb, sigb, forcing):
        for c in range(ref.shape[0]):
            for r in (0, PAD + R + DEEP):
                ref[c, r : r + DEEP, :] = jnp.zeros((DEEP, C), jnp.float32)
    for ref in (turned, pack, f_strip, f_out):
        ref[...] = jnp.zeros_like(ref)

    for copy in loads[:5]:
        copy.wait()
    fields = [velb.at[0], velb.at[1], sigb.at[0], sigb.at[1], sigb.at[2], mass, strength, mask]
    for q, field in enumerate(fields):
        t = field[PAD : PAD + R, :].astype(jnp.float32).T
        low[q] = t[0:DEEP]
        high[q] = t[C - DEEP : C]
    loads[5].wait()
    for c in range(G):
        t = bands[:, :, c * C : (c + 1) * C].reshape(4 * B, C).T
        f_out[(c + 1) % G, 0:DEEP, 0 : 4 * B] = t[C - DEEP : C]
        f_out[(c + G - 1) % G, DEEP : 2 * DEEP, 0 : 4 * B] = t[0:DEEP]
    f_in[gx] = f_out[gx]

    pl.semaphore_wait(barrier, len(partners))

    near, far = pl.ds(0, DEEP), pl.ds(DEEP, DEEP)
    centre, before, after = pl.ds(SIDE, R), pl.ds(0, SIDE), pl.ds(SIDE + R, SIDE)
    first, final_rows = pl.ds(0, SIDE), pl.ds(R - SIDE, SIDE)
    plan = (
        (WEST, low, strip.at[:, far, centre]),
        (EAST, high, strip.at[:, near, centre]),
        (SW, low.at[:, :, first], strip.at[:, far, after]),
        (SE, high.at[:, :, first], strip.at[:, near, after]),
        (NW, low.at[:, :, final_rows], strip.at[:, far, before]),
        (NE, high.at[:, :, final_rows], strip.at[:, near, before]),
    )
    started = []
    for n, (way, src, dst) in enumerate(plan):
        started.append(remote(src, dst, h_send.at[n], h_recv.at[n], at(*STEPS[way])))
    bottom, top = pl.ds(PAD, DEEP), pl.ds(PAD + R - DEEP, DEEP)
    under, over = pl.ds(PAD - DEEP, DEEP), pl.ds(PAD + R, DEEP)
    for n, ref in enumerate((velb, sigb, mass, strength, mask)):
        for m, (way, src, dst) in enumerate(((SOUTH, bottom, over), (NORTH, top, under))):
            a, b = (ref.at[:, src], ref.at[:, dst]) if len(ref.shape) == 3 else (ref.at[src], ref.at[dst])
            started.append(remote(a, b, y_send.at[2 * n + m], y_recv.at[2 * n + m], at(*STEPS[way])))

    mine = pl.ds(pl.multiple_of(gx * B, B), B)
    padded_mine = pl.ds(pl.multiple_of(PAD + gx * B, DEEP), B)
    own_columns = pl.ds(pl.multiple_of(gx * C, C), C)
    own_forcing = pltpu.make_async_copy(bands.at[:, :, own_columns], forcing.at[:, padded_mine], f_recv.at[0])
    for d in sorted(range(1, G), key=lambda d: -abs(2 * d - G)):
        to = lax.rem(gx + d, G)
        columns = pl.ds(pl.multiple_of(to * C, C), C)
        started.append(remote(bands.at[:, :, columns], forcing.at[:, padded_mine], f_send.at[d], f_recv.at[d], at(d, 0)))
        started.append(remote(f_out.at[to], f_in.at[gx], s_send.at[d], s_recv.at[d], at(d, 0)))
    for copy in started:
        copy.start()
    own_forcing.start()

    def beyond(side):
        step, src, dst = ((1, pl.ds(B - DEEP, DEEP), under), (-1, near, over))[side]
        copies = []
        for d in range(G):
            where = {"gx": d, "gy": lax.rem(gy + step + Y, Y)}
            k = 2 * side
            copies.append(
                remote(bands.at[:, src, pl.ds(d * C, C)], forcing.at[:, dst], e_send.at[d, k], e_recv.at[k], where)
            )
            copies.append(remote(f_out.at[d], f_in.at[G + side], e_send.at[d, k + 1], e_recv.at[k + 1], where))
        return copies

    edges = ((G - 1, 0), (0, 1))
    for holder, side in edges:

        @pl.when(gx == holder)
        def _():
            for copy in beyond(side):
                copy.start()

    for copy in started[:16]:
        copy.wait_recv()
    for copy in started[6:16]:
        copy.wait_send()

    has_south = (gy > 0).astype(jnp.float32)
    has_north = (gy < Y - 1).astype(jnp.float32)
    for c in range(2):
        velb[c, under, :] = velb[c, under, :] * has_south
        velb[c, over, :] = velb[c, over, :] * has_north
    ice[...] = mask[...].astype(jnp.float32)
    ice[under, :] = ice[under, :] * has_south
    ice[over, :] = ice[over, :] * has_north
    for c in range(2):
        vel0[c] = velb[c, PAD - DEEP : PAD + R + DEEP, :]

    strip_lane = lax.broadcasted_iota(jnp.int32, (2 * DEEP, L), 1)
    strip_row = lax.broadcasted_iota(jnp.int32, (2 * DEEP, L), 0)
    lat_s = strip_lane - SIDE + gy * R
    inside = ((lat_s >= 0) & (lat_s < R * Y)).astype(jnp.float32)
    cor_s = 0.3 + 1.2 * (lat_s.astype(jnp.float32) + 0.5) / (R * Y)
    sv = [strip[0] * inside, strip[1] * inside]
    sv0 = list(sv)
    ss = [strip[2], strip[3], strip[4]]
    s_strength = strip[6]
    s_ice = strip[7] * inside
    s_inv_mass = 1.0 / strip[5]

    def strip_dx(f, lo, hi):
        right = jnp.where(strip_row == DEEP - 1, lo, pltpu.roll(f, 2 * DEEP - 1, 0))
        left = jnp.where(strip_row == DEEP, hi, pltpu.roll(f, 1, 0))
        return 0.5 * (right - left)

    def strip_dy(f):
        return 0.5 * (pltpu.roll(f, L - 1, 1) - pltpu.roll(f, 1, 1))

    pieces = ((PAD - DEEP, DEEP), (PAD + R, DEEP)) + tuple((PAD + r, R // 2) for r in range(0, R, R // 2))

    def lane_of(n):
        return lax.broadcasted_iota(jnp.int32, (n, C), 1)

    def pack_pair(p, n, a, b):
        lane = lane_of(n)
        pack[p + SHIFT : p + SHIFT + n, :] = jnp.where(
            lane < 1, a, jnp.where(lane < 2, pltpu.roll(a, 2, 1), jnp.where(lane < 3, pltpu.roll(b, 2, 1), pltpu.roll(b, 4, 1)))
        )

    def ring(a, b):
        turned[0:2, :] = a[DEEP - 1 : DEEP + 1]
        turned[2:4, :] = b[DEEP - 1 : DEEP + 1]
        halo[...] = turned[...].T

    def main_dx(f, cols, q, lane):
        right = jnp.where(lane == C - 1, cols[:, q + 1 : q + 2], pltpu.roll(f, C - 1, 1))
        left = jnp.where(lane == 0, cols[:, q : q + 1], pltpu.roll(f, 1, 1))
        return 0.5 * (right - left)

    for p, n in pieces:
        pack_pair(p, n, velb[0, p : p + n, :], velb[1, p : p + n, :])

    sum_lane = lax.broadcasted_iota(jnp.int32, (1, C), 1)
    own_sums = jnp.zeros((1, C), jnp.float32)
    for k in range(ITERS):
        last = k == ITERS - 1
        edge = pack[...].T[0:8]
        ring(sv[0], sv[1])
        for p, n in pieces:
            lane = lane_of(n)
            cols = halo[p + SHIFT : p + SHIFT + n, :]
            slopes = [main_dx(velb[c, p : p + n, :], cols, 2 * c, lane) for c in range(2)]
            slopes += [0.5 * (velb[c, p + 1 : p + n + 1, :] - velb[c, p - 1 : p + n - 1, :]) for c in range(2)]
            new = relaxed(
                *slopes, [sigb[c, p : p + n, :] for c in range(3)], strength[p : p + n, :], ice[p : p + n, :]
            )
            for c in range(3):
                sigb[c, p : p + n, :] = new[c]
            pack_pair(p, n, 0.5 * (new[0] + new[1]), new[2])
        if last:
            keep_sig = pltpu.make_async_copy(sigb.at[:, inner], sig_out, out_sem.at[0])
            keep_sig.start()
        ss = relaxed(
            strip_dx(sv[0], edge[0:1], edge[1:2]), strip_dx(sv[1], edge[2:3], edge[3:4]),
            strip_dy(sv[0]), strip_dy(sv[1]), ss, s_strength, s_ice,
        )
        s_xx = 0.5 * (ss[0] + ss[1])
        edge = pack[...].T[0:8]
        ring(s_xx, ss[2])

        if k == 0:
            own_forcing.wait()
            for copy in started[16:]:
                copy.wait_recv()
            for side in range(2):
                for copy, slot in ((0, forcing.at[:, (under, over)[side]]), (1, f_in.at[G + side])):
                    m = 2 * side + copy
                    remote(slot, slot, e_send.at[0, m], e_recv.at[m], at(0, 1)).wait_recv()
            for f in range(4):
                for b in range(-1, G + 1):
                    slot = G if b < 0 else G + 1 if b == G else b
                    a = SIDE + b * B
                    f_strip[f, :, a : a + B] = f_in[slot, :, f * B : (f + 1) * B]

        total = jnp.zeros((R // 2, C), jnp.float32)
        for p, n in pieces:
            if last and n == DEEP:
                continue
            lane = lane_of(n)
            cols = halo[p + SHIFT : p + SHIFT + n, :]
            sxx = 0.5 * (sigb[0, p : p + n, :] + sigb[1, p : p + n, :])
            sxy = sigb[2, p : p + n, :]
            hi, lo = pl.ds(p + 1, n), pl.ds(p - 1, n)
            dy_xy = 0.5 * (sigb[2, hi, :] - sigb[2, lo, :])
            dy_yy = 0.25 * ((sigb[0, hi, :] - sigb[1, hi, :]) - (sigb[0, lo, :] - sigb[1, lo, :]))
            force_east = main_dx(sxx, cols, 0, lane) + dy_xy
            force_north = main_dx(sxy, cols, 2, lane) + dy_yy
            u, v = velb[0, p : p + n, :], velb[1, p : p + n, :]
            fe, fn, cu, cv = (forcing[c, p : p + n, :] for c in range(4))
            frac = ice[p : p + n, :]
            if k == 0:
                inv_mass = 1.0 / mass[p : p + n, :]
                mass[p : p + n, :] = inv_mass
            else:
                inv_mass = mass[p : p + n, :]
            lat = (gy * R + (p - PAD) + lax.broadcasted_iota(jnp.int32, (n, C), 0)).astype(jnp.float32)
            coriolis = 0.3 + 1.2 * (lat + 0.5) / (R * Y)
            start = [vel0[c, p - PAD + DEEP : p - PAD + DEEP + n, :] for c in range(2)]
            new_u, new_v = moved(u, v, start, force_east, force_north, fe, fn, cu, cv, inv_mass, coriolis, frac)
            velb[0, p : p + n, :] = new_u
            velb[1, p : p + n, :] = new_v
            if last:
                drag = drag_of(new_u, new_v, cu, cv) * frac
                ocean[0, p - PAD : p - PAD + n, :] = drag * (new_u - cu)
                ocean[1, p - PAD : p - PAD + n, :] = drag * (new_v - cv)
            else:
                pack_pair(p, n, new_u, new_v)
            if n > DEEP:
                du = new_u - u
                dv = new_v - v
                total = total + (du * du + dv * dv)
        own_sums = jnp.where(sum_lane == k, jnp.sum(total), own_sums)
        if not last:
            s_yy = 0.5 * (ss[0] - ss[1])
            force_east = strip_dx(s_xx, edge[0:1], edge[1:2]) + strip_dy(ss[2])
            force_north = strip_dx(ss[2], edge[2:3], edge[3:4]) + strip_dy(s_yy)
            sv = list(
                moved(
                    sv[0], sv[1], sv0, force_east, force_north,
                    f_strip[0], f_strip[1], f_strip[2], f_strip[3], s_inv_mass, cor_s, s_ice,
                )
            )

    rs[...] = own_sums
    here = gx * Y + gy
    sums = []
    for n, (dx, dy) in enumerate(partners):
        copy = remote(rs, rx.at[here], r_send.at[n], r_recv.at[n], at(dx, dy))
        copy.start()
        sums.append(copy)
    rx[here] = own_sums
    outs = []
    for d in sorted(range(1, G), key=lambda d: -abs(2 * d - G)):
        to = lax.rem(gx + d, G)
        copy = pltpu.make_async_remote_copy(
            src_ref=ocean.at[:, pl.ds(pl.multiple_of(to * B, B), B)],
            dst_ref=os_out.at[:, :, own_columns],
            send_sem=o_send.at[d], recv_sem=o_recv.at[d],
            device_id={"gx": to, "gy": gy}, device_id_type=MESH,
        )
        copy.start()
        outs.append(copy)
    own_out = pltpu.make_async_copy(ocean.at[:, mine], os_out.at[:, :, own_columns], out_sem.at[1])
    own_out.start()
    keep_vel = pltpu.make_async_copy(velb.at[:, inner], vel_out, out_sem.at[2])
    keep_vel.start()
    for copy in sums:
        copy.wait_recv()
    total = jnp.sum(rx[...], axis=0)
    for k in range(ITERS):
        res_out[k] = jnp.sum(jnp.where(sum_lane == k, total, 0.0))
    for copy in outs:
        copy.wait_recv()
    for copy in started[:6] + started[16:] + outs + sums:
        copy.wait_send()
    for holder, side in edges:

        @pl.when(gx == holder)
        def _():
            for copy in beyond(side):
                copy.wait_send()

    own_out.wait()
    keep_vel.wait()
    keep_sig.wait()


def local(velocity, stress, ice_mass, strength, land_mask, ocean_forcing):
    G, Y = lax.axis_size("gx"), lax.axis_size("gy")
    R, C = velocity.shape[1:]
    B = ocean_forcing.shape[1]
    L = R + 2 * SIDE
    f32 = jnp.float32
    dma = pltpu.SemaphoreType.DMA
    any_space = pl.BlockSpec(memory_space=pl.ANY)
    return pl.pallas_call(
        functools.partial(kernel, G, Y, R, C, B),
        out_shape=(
            jax.ShapeDtypeStruct(velocity.shape, f32),
            jax.ShapeDtypeStruct(stress.shape, f32),
            jax.ShapeDtypeStruct((ITERS,), f32),
            jax.ShapeDtypeStruct((2,) + ocean_forcing.shape[1:], f32),
        ),
        in_specs=[any_space] * 6,
        out_specs=(any_space, any_space, pl.BlockSpec(memory_space=pltpu.SMEM), any_space),
        scratch_shapes=[
            pltpu.VMEM((2, R + 2 * DEEP, C), f32),
            pltpu.VMEM((2, R + 2 * PAD, C), f32),
            pltpu.VMEM((3, R + 2 * PAD, C), f32),
            pltpu.VMEM((R + 2 * PAD, C), f32),
            pltpu.VMEM((R + 2 * PAD, C), f32),
            pltpu.VMEM((R + 2 * PAD, C), f32),
            pltpu.VMEM((R + 2 * PAD, C), jnp.int32),
            pltpu.VMEM(ocean_forcing.shape, f32),
            pltpu.VMEM((4, R + 2 * PAD, C), f32),
            pltpu.VMEM((2, R, C), f32),
            pltpu.VMEM((L, C), f32),
            pltpu.VMEM((L, C), f32),
            pltpu.VMEM((C, L), f32),
            pltpu.VMEM((8, DEEP, R), f32),
            pltpu.VMEM((8, DEEP, R), f32),
            pltpu.VMEM((8, 2 * DEEP, L), f32),
            pltpu.VMEM((G, 2 * DEEP, SIDE), f32),
            pltpu.VMEM((G + 2, 2 * DEEP, SIDE), f32),
            pltpu.VMEM((4, 2 * DEEP, L), f32),
            pltpu.VMEM((1, C), f32),
            pltpu.VMEM((G * Y, 1, C), f32),
            dma((6,)),
            dma((G,)),
            dma((G,)),
            dma((G,)),
            dma((G,)),
            dma((G, 4)),
            dma((4,)),
            dma((6,)),
            dma((6,)),
            dma((10,)),
            dma((10,)),
            dma((G,)),
            dma((G,)),
            dma((G * Y,)),
            dma((G * Y,)),
            dma((3,)),
        ],
        compiler_params=pltpu.CompilerParams(collective_id=0, has_side_effects=True),
    )(velocity, stress, ice_mass, strength, land_mask, ocean_forcing)


def solution(mesh):
    placed = (
        P(None, "gy", "gx"),
        P(None, "gy", "gx"),
        P("gy", "gx"),
        P("gy", "gx"),
        P("gy", "gx"),
        P(None, ("gy", "gx"), None),
    )
    return jax.shard_map(
        local,
        mesh=mesh,
        in_specs=placed,
        out_specs=(P(None, "gy", "gx"), P(None, "gy", "gx"), P(), P(None, ("gy", "gx"), None)),
        check_vma=False,
    )
```
